32 devices in a mesh: dp: 8 (over z, y), mp: 4 (over x, core).
Axes of the slice: x: 2, y: 2, z: 4, core: 2. Of those that a mesh axis runs over, the one named last changes fastest.
Arguments:
- tokens: bfloat16 [49152, 512], P('dp'), may hold values from -6 to 6
- w_uvqk: bfloat16 [512, 2048], P(None, 'mp')
- w_out: bfloat16 [512, 512], replicated, may hold values from -0.25 to 0.25
- hist_len: int32 [8, 24], P('dp'), may hold values from 64 to 256, as said below
- owner: int32 [8, 24], P('dp'), may hold values from 0 to 7, as said below
- recv_offset: int32 [8, 24], P('dp'), may hold values from 0 to 47, as said below
- block_start: int32 [8, 24], P('dp'), may hold values from 0 to 47, as said below
Outputs:
- packed_out: bfloat16 [49152, 512], P('dp', 'mp')
- user_state: bfloat16 [192, 512], P('dp', 'mp')
The draws below stay inside these ranges and needn't reach their ends.
Inputs may be any that keep to these rules, and one draw needn't show every extreme that they name: User (d, u) has ceil(hist_len / 128) blocks, at most 2. owner[d, u] = (p(d) + r(u mod 8)) mod 8 for two permutations p, r of the indices of dp drawn from the seed: every owner receives exactly 24 users, and one device sends at most 3 users to one owner. On some owner every received user has 2 blocks. `recv_offset`: the users of one owner occupy disjoint runs of its 48 blocks, in the order of u; on some owner they fill all 48 blocks. `block_start`: the users of one device occupy disjoint runs of its 48 blocks, in the order of u.
All inputs are finite; a program needn't handle non-finite values.
Results may differ from the reference program's by a relative error of at most 0.0059.
Values may be sent and summed in bfloat16 or wider, within the bound.
No kernel may reach another device: no remote copies, remote signals or barrier semaphores. Data moves between devices by JAX's collectives and lax.ppermute only.
A program may use at most 128 MiB of HBM per device.

```python
import jax
import jax.numpy as jnp
from jax import lax

D = 512
HEADS = 4
BLOCK = 128
MAXB = 2
USERS_DEV = 24
BLK_DEV = 48
ROWS = 49152
N_DP = 8


def place_runs(key, run_sizes, salt_value):
    before = jnp.cumsum(run_sizes, axis=1) - run_sizes
    spare_blocks = BLK_DEV - jnp.sum(run_sizes, axis=1, keepdims=True)
    gap_sums = jnp.cumsum(jax.random.randint(jax.random.fold_in(key, salt_value), run_sizes.shape, 0, 2), axis=1)
    return (before + jnp.minimum(gap_sums, spare_blocks)).astype(jnp.int32)


def draw_tables(key):
    device_count = N_DP
    user_count = USERS_DEV
    dev_perm = jax.random.permutation(jax.random.fold_in(key, 101), device_count).astype(jnp.int32)
    user_perm = jax.random.permutation(jax.random.fold_in(key, 102), device_count).astype(jnp.int32)
    user_ids = jnp.arange(user_count, dtype=jnp.int32)
    shifts = user_perm[user_ids % device_count]
    owners = ((dev_perm[:, None] + shifts[None, :]) % device_count).astype(jnp.int32)
    hottest = jax.random.randint(jax.random.fold_in(key, 103), (), 0, device_count)
    coin_flip = jax.random.randint(jax.random.fold_in(key, 104), (device_count, user_count), 0, 4)
    small_count = jax.random.randint(jax.random.fold_in(key, 108), (device_count, user_count), 1, MAXB + 1)
    counts = jnp.where(coin_flip > 0, MAXB, small_count)
    counts = jnp.where(owners == hottest, MAXB, counts).astype(jnp.int32)
    least_tail = jnp.where(counts == 1, BLOCK // 2, 1)
    extra_rows = jax.random.randint(jax.random.fold_in(key, 105), (device_count, user_count), 0, BLOCK + 1)
    last_fill = least_tail + extra_rows % (BLOCK + 1 - least_tail)
    lengths = ((counts - 1) * BLOCK + last_fill).astype(jnp.int32)
    starts = place_runs(key, counts, 106)
    inverse = jnp.zeros((device_count,), jnp.int32).at[dev_perm].set(jnp.arange(device_count, dtype=jnp.int32))
    sources = inverse[(jnp.arange(device_count, dtype=jnp.int32)[:, None] - shifts[None, :]) % device_count]
    incoming = counts[sources, user_ids[None, :]]
    landing = place_runs(key, incoming, 107)
    offsets = landing[owners, user_ids[None, :]].astype(jnp.int32)
    return (lengths, owners, offsets, starts)


def draw_hist_len(key, part):
    return draw_tables(key)[0]


def draw_owner(key, part):
    return draw_tables(key)[1]


def draw_recv_offset(key, part):
    return draw_tables(key)[2]


def draw_block_start(key, part):
    return draw_tables(key)[3]


def draw_w_uvqk(key, part):
    base_draw = jax.random.normal(jax.random.fold_in(key, 1), (D, 4 * D), jnp.float32)
    log_scale = jax.random.uniform(jax.random.fold_in(key, 2), (1, 4 * D), jnp.float32, -1.2, 1.2)
    return (base_draw * jnp.exp(log_scale) / jnp.sqrt(D * 1.0)).astype(jnp.bfloat16)


def shard_levels(rng, extent, split, least, high):
    factor_of = 1.0
    for dim, parts in split:
        steps = jax.random.uniform(jax.random.fold_in(jax.random.fold_in(rng, 6), dim), (parts,), jnp.float32, least / len(split), high / len(split))
        factor_of = factor_of * jnp.repeat(jnp.exp(steps), extent[dim] // parts).reshape((-1,) + (1,) * (len(extent) - 1 - dim))
    return factor_of


def normal_values(key, extent, spread, bound, split=(), held_as=jnp.bfloat16):
    values = jax.random.normal(key, extent, jnp.float32) * spread
    if len(split) > 0:
        values = shard_levels(key, extent, split, -0.22, 0.18) * values
    return jnp.clip(values, min=-bound, max=bound).astype(held_as)


def setup_inputs(seed: int = 0) -> dict:
    key_of = jax.random.split(jax.random.key(seed), 8)
    tokens = normal_values(key_of[0], (ROWS, D), 1.0, 6.0, ((0, 8),))
    w_uvqk = draw_w_uvqk(jax.random.fold_in(key_of[7], 71), 0)
    w_out = normal_values(key_of[2], (D, D), D ** -0.5, 0.25)
    hist_len = draw_hist_len(jax.random.fold_in(key_of[7], 71), 0)
    owner = draw_owner(jax.random.fold_in(key_of[7], 71), 0)
    recv_offset = draw_recv_offset(jax.random.fold_in(key_of[7], 71), 0)
    block_start = draw_block_start(jax.random.fold_in(key_of[7], 71), 0)
    return dict(tokens=tokens, w_uvqk=w_uvqk, w_out=w_out, hist_len=hist_len, owner=owner, recv_offset=recv_offset, block_start=block_start)


EPS = 1e-05

def norm_rows(values):
    average = lax.optimization_barrier(jnp.mean(values, axis=-1, keepdims=True))
    variance = lax.optimization_barrier(jnp.mean(values * values, axis=-1, keepdims=True)) - average * average
    return (values - average) * lax.rsqrt(variance + EPS)

def rounded(values):
    return lax.optimization_barrier(values.astype(jnp.bfloat16)).astype(jnp.float32)

def reference(tokens, w_uvqk, w_out, hist_len, owner, recv_offset, block_start):
    head_size = D // HEADS
    window_rows = MAXB * BLOCK
    total_rows = tokens.shape[0]
    device_count = hist_len.shape[0]
    user_count = hist_len.shape[1]
    padded = jnp.concatenate([tokens, jnp.zeros((window_rows, D), tokens.dtype)], 0)
    position = jnp.arange(window_rows, dtype=jnp.int32)
    causal = position[None, :] <= position[:, None]
    device_ids = (jnp.arange(device_count * user_count, dtype=jnp.int32) // user_count).astype(jnp.int32)
    flat_len = hist_len.reshape(-1).astype(jnp.int32)
    flat_start = block_start.reshape(-1).astype(jnp.int32)
    flat_owner = owner.reshape(-1).astype(jnp.int32)
    flat_offset = recv_offset.reshape(-1).astype(jnp.int32)

    def one_user(user_item):
        device_id, length, start = user_item
        first_row = ((device_id * BLK_DEV + start) * BLOCK).astype(jnp.int32)
        rows_in = lax.dynamic_slice_in_dim(padded, first_row, window_rows, 0)
        widened = rows_in.astype(jnp.float32)
        normed = norm_rows(widened).astype(jnp.bfloat16)
        projected = jax.nn.silu(jnp.dot(normed, w_uvqk, preferred_element_type=jnp.float32))
        pieces = rounded(projected).reshape(window_rows, HEADS, 4, head_size)
        raw_scores = jnp.einsum('ihd,jhd->hij', pieces[:, :, 2], pieces[:, :, 3]) * head_size ** (-0.5)
        allowed = causal & (position[None, :] < length)
        weights = rounded(jnp.where(allowed[None], jax.nn.silu(raw_scores) / window_rows, 0.0))
        attended = jnp.einsum('hij,jhd->ihd', weights, pieces[:, :, 1]).reshape(window_rows, D)
        gated_rows = (norm_rows(attended) * pieces[:, :, 0].reshape(window_rows, D)).astype(jnp.bfloat16)
        mixed_rows = jnp.dot(gated_rows, w_out, preferred_element_type=jnp.float32) + widened
        return mixed_rows.astype(jnp.bfloat16)
    outputs = lax.map(one_user, (device_ids, flat_len, flat_start))
    targets = ((flat_owner * BLK_DEV + flat_offset) * BLOCK)[:, None] + position[None, :]
    targets = jnp.where(position[None, :] < flat_len[:, None], targets, total_rows).astype(jnp.int32)
    packed = jnp.zeros((total_rows + 1, D), jnp.bfloat16)
    packed = packed.at[targets.reshape(-1)].set(outputs.reshape(-1, D))[:total_rows]
    user_state = outputs[jnp.arange(device_count * user_count, dtype=jnp.int32), flat_len - 1]
    return (packed, user_state)
```

```python
import functools

import jax
import jax.numpy as jnp
from jax import lax
from jax.experimental import pallas as pl
from jax.experimental.pallas import tpu as pltpu
from jax.sharding import PartitionSpec as P

BLOCK = 128
MAXB = 2
HEAD = 128
WINDOW = MAXB * BLOCK
EPS = 1e-05


def half_silu(half):
    return half + half * jnp.tanh(half)


def norm_scale(total, squares, width):
    average = total * (1.0 / width)
    variance = squares * (1.0 / width) - average * average
    return average, lax.rsqrt(variance + EPS)


def layer_kernel(mp, groups, table_ref, *refs):
    block_refs = refs[:MAXB]
    w_refs = refs[MAXB : MAXB + mp]
    wo_ref = refs[MAXB + mp]
    out_refs = refs[MAXB + mp + 1 : MAXB + 2 * mp + 1]
    state_ref = refs[MAXB + 2 * mp + 1]
    mixed_ref = refs[MAXB + 2 * mp + 2]
    slot = pl.program_id(0)
    mine = table_ref[0]
    length = table_ref[1 + groups * 0 + slot]
    width = wo_ref.shape[0]
    widened = jnp.concatenate([ref[...] for ref in block_refs], 0).astype(jnp.float32)
    average, scale = norm_scale(
        jnp.sum(widened, 1, keepdims=True), jnp.sum(widened * widened, 1, keepdims=True), width
    )
    normed = ((widened - average) * scale).astype(jnp.bfloat16)
    row = lax.broadcasted_iota(jnp.int32, (BLOCK, BLOCK), 0)
    col = lax.broadcasted_iota(jnp.int32, (BLOCK, BLOCK), 1)
    causal = col <= row
    local = w_refs[0].shape[1] // (4 * HEAD)
    half_scale = 0.5 * HEAD ** (-0.5)
    attended, gates = [], []
    total = jnp.zeros((WINDOW, 1), jnp.float32)
    squares = jnp.zeros((WINDOW, 1), jnp.float32)
    for w_ref in w_refs:
        for head in range(local):
            cols = slice(head * 4 * HEAD, (head + 1) * 4 * HEAD)
            half = 0.5 * jnp.dot(normed, w_ref[:, cols], preferred_element_type=jnp.float32)
            proj = half_silu(half).astype(jnp.bfloat16)
            u, v, q, k = (proj[:, i * HEAD : (i + 1) * HEAD] for i in range(4))
            pieces = []
            for b in range(MAXB):
                rows = slice(b * BLOCK, (b + 1) * BLOCK)
                seen = slice(0, (b + 1) * BLOCK)
                raw = lax.dot_general(
                    q[rows], k[seen], (((1,), (1,)), ((), ())), preferred_element_type=jnp.float32
                )
                act = half_silu(raw * half_scale) * (1.0 / WINDOW)
                last = jnp.where(causal, act[:, b * BLOCK :], 0.0)
                act = last if b == 0 else jnp.concatenate([act[:, : b * BLOCK], last], 1)
                pieces.append(
                    jnp.dot(act.astype(jnp.bfloat16), v[seen], preferred_element_type=jnp.float32)
                )
            value = jnp.concatenate(pieces, 0)
            total += jnp.sum(value, 1, keepdims=True)
            squares += jnp.sum(value * value, 1, keepdims=True)
            attended.append(value)
            gates.append(u.astype(jnp.float32))
    average, scale = norm_scale(total, squares, width)
    mixed = widened
    part = local * HEAD
    for s in range(mp):
        gated = jnp.concatenate(
            [
                ((attended[s * local + h] - average) * scale * gates[s * local + h]).astype(
                    jnp.bfloat16
                )
                for h in range(local)
            ],
            1,
        )
        start = pl.multiple_of((mine ^ s) * part, part)
        mixed += jnp.dot(gated, wo_ref[pl.ds(start, part), :], preferred_element_type=jnp.float32)
    live = lax.broadcasted_iota(jnp.int32, (WINDOW, 1), 0)
    mixed = jnp.where(live < length, mixed, 0.0).astype(jnp.bfloat16).astype(jnp.float32)
    last_row = jnp.sum(jnp.where(live == length - 1, mixed, 0.0), 0, keepdims=True)
    quarter = width // mp
    mixed_ref[:WINDOW, :] = mixed
    mixed_ref[WINDOW : WINDOW + 8, :] = jnp.broadcast_to(last_row, (8, width))
    for s in range(mp):
        start = pl.multiple_of((mine ^ s) * quarter, quarter)
        out_refs[s][...] = mixed_ref[:WINDOW, pl.ds(start, quarter)].astype(jnp.bfloat16)
        state_ref[s] = mixed_ref[WINDOW : WINDOW + 8, pl.ds(start, quarter)]


def run_layer(table, tokens, shards, w_out, groups):
    mp = len(shards)
    width = tokens.shape[1]
    quarter = width // mp
    top = tokens.shape[0] // BLOCK - 1

    def block_map(b, slot, table_ref):
        return (jnp.minimum(table_ref[1 + groups + slot] + b, top), 0)

    def whole(slot, table_ref):
        return (0, 0)

    outs = pl.pallas_call(
        functools.partial(layer_kernel, mp, groups),
        grid_spec=pltpu.PrefetchScalarGridSpec(
            num_scalar_prefetch=1,
            grid=(groups,),
            in_specs=[
                pl.BlockSpec((BLOCK, width), functools.partial(block_map, b)) for b in range(MAXB)
            ]
            + [pl.BlockSpec(w.shape, whole) for w in shards]
            + [pl.BlockSpec(w_out.shape, whole)],
            out_specs=[
                pl.BlockSpec((WINDOW, quarter), lambda slot, table_ref: (slot, 0))
                for _ in range(mp)
            ]
            + [pl.BlockSpec((mp, None, 8, quarter), lambda slot, table_ref: (0, slot, 0, 0))],
            scratch_shapes=[pltpu.VMEM((WINDOW + 8, width), jnp.float32)],
        ),
        out_shape=[
            jax.ShapeDtypeStruct((groups * WINDOW, quarter), jnp.bfloat16) for _ in range(mp)
        ]
        + [jax.ShapeDtypeStruct((mp, groups, 8, quarter), jnp.float32)],
        name="layer_rows",
    )(table, *([tokens] * MAXB), *shards, w_out)
    return outs[:mp], outs[mp]


def place_kernel(count, slots, order_ref, *refs):
    in_refs = refs[:count]
    state_refs = refs[count : count + slots]
    out_ref, user_ref, zero_ref, taken_ref, users_ref, sem = refs[count + slots :]
    blocks = out_ref.shape[0] // BLOCK
    per = in_refs[0].shape[0] // WINDOW
    zero_ref[...] = jnp.zeros_like(zero_ref)

    def clear(i, c):
        taken_ref[i] = 0
        return c

    lax.fori_loop(0, blocks, clear, 0)
    for i in range(count):
        for k in range(per):
            offset = order_ref[0, i * per + k]
            length = order_ref[1, i * per + k]
            for b in range(MAXB):

                @pl.when(length > b * BLOCK)
                def _():
                    taken_ref[offset + b] = 1
                    pltpu.make_async_copy(
                        in_refs[i].at[pl.ds(k * WINDOW + b * BLOCK, BLOCK), :],
                        out_ref.at[pl.ds((offset + b) * BLOCK, BLOCK), :],
                        sem,
                    ).start()

    def fill(i, c):
        @pl.when(taken_ref[i] == 0)
        def _():
            pltpu.make_async_copy(
                zero_ref, out_ref.at[pl.ds(i * BLOCK, BLOCK), :], sem
            ).start()

        return c

    lax.fori_loop(0, blocks, fill, 0)
    users_ref[...] = jnp.zeros_like(users_ref)
    groups = state_refs[0].shape[0]
    for s in range(slots):
        for g in range(groups):
            length = order_ref[3, s * groups + g]

            @pl.when(length > 0)
            def _():
                users_ref[pl.ds(order_ref[2, s * groups + g], 1), :] = state_refs[s][g, 0:1, :]

    user_ref[...] = users_ref[...].astype(user_ref.dtype)
    pltpu.make_async_copy(out_ref, out_ref, sem).wait()


def place(order, arrived, states, rows, users):
    quarter = arrived[0].shape[1]
    anywhere = pl.BlockSpec(memory_space=pl.ANY)
    return pl.pallas_call(
        functools.partial(place_kernel, len(arrived), len(states)),
        in_specs=[pl.BlockSpec(memory_space=pltpu.SMEM)]
        + [anywhere] * len(arrived)
        + [pl.BlockSpec(memory_space=pltpu.VMEM)] * len(states),
        out_specs=[anywhere, pl.BlockSpec(memory_space=pltpu.VMEM)],
        out_shape=[
            jax.ShapeDtypeStruct((rows, quarter), jnp.bfloat16),
            jax.ShapeDtypeStruct((users, quarter), jnp.bfloat16),
        ],
        scratch_shapes=[
            pltpu.VMEM((BLOCK, quarter), jnp.bfloat16),
            pltpu.SMEM((rows // BLOCK,), jnp.int32),
            pltpu.VMEM((users, quarter), jnp.float32),
            pltpu.SemaphoreType.DMA(()),
        ],
        name="place_blocks",
    )(order, *arrived, *states)


def per_device(dp, mp, tokens, w_uvqk, w_out, hist_len, owner, recv_offset, block_start):
    users = hist_len.shape[1]
    per_pair = -(-users // dp)
    chunk = -(-users // per_pair)
    rounds = dp // mp
    me, mine = lax.axis_index("dp"), lax.axis_index("mp")

    def delta(e, m):
        return e * mp + ((m >> 1) ^ ((m & 1) * (mp - 1)))

    def swap(value, j):
        return lax.ppermute(value, "mp", [(i, i ^ j) for i in range(mp)])

    def send(value, e, j):
        pairs = [
            (d * mp + m, (d ^ delta(e, m)) * mp + (m ^ j)) for d in range(dp) for m in range(mp)
        ]
        return lax.ppermute(value, ("dp", "mp"), pairs)

    far = {0: w_uvqk}
    hop = mp // 2
    while hop >= 1:
        far.update({s + hop: swap(value, hop) for s, value in list(far.items())})
        hop //= 2
    shards = [far[s] for s in range(mp)]

    user_ids = jnp.arange(users, dtype=jnp.int32)
    chosen = (owner[0][None, None, :] == jnp.arange(dp, dtype=jnp.int32)[:, None, None]) & (
        (user_ids // chunk)[None, None, :] == jnp.arange(per_pair, dtype=jnp.int32)[None, :, None]
    )
    facts = jnp.stack([hist_len[0], recv_offset[0], block_start[0], user_ids])
    pairs = jnp.sum(jnp.where(chosen[:, :, None, :], facts[None, None], 0), -1)
    coming = lax.all_to_all(
        pairs[:, :, :2].reshape(dp, per_pair * 2), "dp", 0, 0, tiled=True
    ).reshape(dp, per_pair, 2)

    owners = [[me ^ delta(e, mine ^ j) for j in range(mp)] for e in range(rounds)]
    arrived, order = [], []
    states = []
    results = []
    for e in reversed(range(rounds)):
        own = jnp.take(pairs, owners[e][0], axis=0)
        table = jnp.concatenate([mine[None].astype(jnp.int32), own[:, 0], own[:, 2]])
        outs, state = run_layer(table, tokens, shards, w_out, per_pair)
        results.append((e, outs, state))
    order_index = []
    for e, outs, state in results:
        for j in range(mp):
            arrived.append(send(outs[j], e, j))
            order_index.append(owners[e][j])
    all_state = [jnp.concatenate([st[j] for _, _, st in results], 0) for j in range(mp)]
    states = [all_state[0]] + [swap(all_state[j], j) for j in range(1, mp)]
    land = jnp.take(coming, jnp.stack(order_index), axis=0).reshape(-1, 2)
    state_index = jnp.stack([owners[e][j] for j in range(mp) for e, _, _ in results])
    home = jnp.take(pairs, state_index, axis=0).reshape(-1, 4)
    order = jnp.stack([land[:, 1], land[:, 0], home[:, 3], home[:, 0]])
    return place(order, arrived, states, tokens.shape[0], users)


def solution(mesh):
    dp, mp = mesh.shape["dp"], mesh.shape["mp"]
    in_specs = (
        P("dp", None),
        P(None, "mp"),
        P(),
        P("dp", None),
        P("dp", None),
        P("dp", None),
        P("dp", None),
    )
    out_specs = (P("dp", "mp"), P("dp", "mp"))
    return jax.shard_map(
        functools.partial(per_device, dp, mp),
        mesh=mesh,
        in_specs=in_specs,
        out_specs=out_specs,
        check_vma=False,
    )
```

```python
import functools

import jax
import jax.numpy as jnp
from jax import lax
from jax.experimental import pallas as pl
from jax.experimental.pallas import tpu as pltpu
from jax.sharding import PartitionSpec as P


BLOCK = 128
MAXB = 2
HEAD = 128
WINDOW = MAXB * BLOCK
TAIL = 8
EPS = 1e-05
LIMIT = pltpu.CompilerParams(vmem_limit_bytes=24 * 1024 * 1024)


def in_vmem(value):
    return pltpu.with_memory_space_constraint(value, pltpu.VMEM)


def in_hbm(value):
    return pltpu.with_memory_space_constraint(value, pltpu.HBM)


def half_silu(half):
    return half + half * jnp.tanh(half)


def norm_scale(total, squares, width):
    average = total * (1.0 / width)
    variance = squares * (1.0 / width) - average * average
    return average, lax.rsqrt(variance + EPS)


def norm_half(widened):
    average, scale = norm_scale(
        jnp.sum(widened, 1, keepdims=True),
        jnp.sum(widened * widened, 1, keepdims=True),
        widened.shape[1],
    )
    return ((widened - average) * (0.5 * scale)).astype(jnp.bfloat16)


def attend_heads(halved, w_refs):
    row = lax.broadcasted_iota(jnp.int32, (BLOCK, BLOCK), 0)
    col = lax.broadcasted_iota(jnp.int32, (BLOCK, BLOCK), 1)
    causal = col <= row
    half_scale = 0.5 * HEAD ** (-0.5)
    values, gates = [], []
    for w_ref in w_refs:
        for head in range(w_ref.shape[1] // (4 * HEAD)):
            cols = slice(head * 4 * HEAD, (head + 1) * 4 * HEAD)
            half = jnp.dot(halved, w_ref[:, cols], preferred_element_type=jnp.float32)
            proj = half_silu(half).astype(jnp.bfloat16)
            u, v, q, k = (proj[:, i * HEAD : (i + 1) * HEAD] for i in range(4))
            raw = lax.dot_general(q, k, (((1,), (1,)), ((), ())), preferred_element_type=jnp.float32)
            weights = []
            for b in range(MAXB):
                rows = slice(b * BLOCK, (b + 1) * BLOCK)
                act = half_silu(raw[rows, : (b + 1) * BLOCK] * half_scale)
                pieces = [act[:, : b * BLOCK]] if b > 0 else []
                pieces.append(jnp.where(causal, act[:, b * BLOCK :], 0.0))
                if b + 1 < MAXB:
                    pieces.append(jnp.zeros((BLOCK, WINDOW - (b + 1) * BLOCK), jnp.float32))
                weights.append(jnp.concatenate(pieces, 1).astype(jnp.bfloat16))
            values.append(
                jnp.dot(jnp.concatenate(weights, 0), v, preferred_element_type=jnp.float32)
            )
            gates.append(u)
    return values, gates


def near_rows(base, widened, w_refs, out_refs):
    rows_ref, half_ref, value_ref, gate_ref = out_refs
    rows = pl.ds(pl.multiple_of(base * WINDOW, WINDOW), WINDOW)
    halved = norm_half(widened)
    rows_ref[rows, :] = widened.astype(rows_ref.dtype)
    half_ref[rows, :] = halved
    values, gates = attend_heads(halved, w_refs)
    value_ref[rows, :] = jnp.concatenate(values, 1)
    gate_ref[rows, :] = jnp.concatenate(gates, 1)


def near_home_kernel(near, total_slots, table_ref, *refs):
    block_refs, w_refs = refs[:MAXB], refs[MAXB : MAXB + near]
    tail_ref = refs[-1]
    slot = pl.program_id(0)
    tail_ref[pl.ds(pl.multiple_of(slot * TAIL, TAIL), TAIL), :] = tail_rows(
        table_ref[slot], table_ref[2 * total_slots + slot], tail_ref.shape[1]
    )
    widened = jnp.concatenate([ref[...] for ref in block_refs], 0).astype(jnp.float32)
    near_rows(slot, widened, w_refs, refs[MAXB + near : -1])


def near_owner_kernel(near, *refs):
    arrived_ref, w_refs = refs[0], refs[1 : 1 + near]
    tail_ref = refs[-1]
    slot = pl.program_id(0)
    first = pl.multiple_of(slot * (WINDOW + TAIL), TAIL)
    tail_ref[pl.ds(pl.multiple_of(slot * TAIL, TAIL), TAIL), :] = arrived_ref[
        pl.ds(first + WINDOW, TAIL), : tail_ref.shape[1]
    ]
    near_rows(slot, arrived_ref[pl.ds(first, WINDOW), :].astype(jnp.float32), w_refs, refs[1 + near : -1])


def far_kernel(mp, far, base, whole, *refs):
    w_refs = refs[:far]
    rows_ref, half_ref, near_value_ref, near_gate_ref, tail_ref, wp_ref = refs[far : far + 6]
    out_refs = refs[far + 6 : -2]
    state_ref, mixed_ref = refs[-2:]
    if whole:
        out_refs = [out_refs[0].at[s] for s in range(mp)]
    slot = pl.program_id(0)
    mine = lax.axis_index("mp")
    width = wp_ref.shape[0]
    rows = pl.ds(pl.multiple_of((base + slot) * WINDOW, WINDOW), WINDOW)
    tail = tail_ref[pl.ds(pl.multiple_of((base + slot) * TAIL, TAIL), TAIL), :]
    length = tail.astype(jnp.float32)[0:1, 0:1]
    values, gates = attend_heads(half_ref[rows, :], w_refs)
    value = jnp.concatenate([near_value_ref[rows, :]] + values, 1)
    gate = jnp.concatenate([near_gate_ref[rows, :]] + gates, 1)
    average, scale = norm_scale(
        jnp.sum(value, 1, keepdims=True) * (1.0 / WINDOW),
        jnp.sum(value * value, 1, keepdims=True) * (1.0 / WINDOW**2),
        width,
    )
    average, scale = average * WINDOW, scale * (1.0 / WINDOW)
    gated = ((value - average) * scale * gate.astype(jnp.float32)).astype(jnp.bfloat16)
    mixed = rows_ref[rows, :].astype(jnp.float32) + jnp.dot(
        gated, wp_ref[...], preferred_element_type=jnp.float32
    )
    live = lax.broadcasted_iota(jnp.int32, (WINDOW, 1), 0).astype(jnp.float32)
    mixed_ref[:WINDOW, :] = jnp.where(live < length, mixed, 0.0)
    final = jnp.sum(jnp.where(live == length - 1.0, mixed, 0.0), 0, keepdims=True)
    mixed_ref[WINDOW:, :] = jnp.broadcast_to(final, (TAIL, width))
    quarter = width // mp
    first = pl.multiple_of(slot * (WINDOW + TAIL), TAIL)
    for s in range(mp):
        start = pl.multiple_of((mine ^ s) * quarter, quarter)
        out_refs[s][pl.ds(first, WINDOW), :] = mixed_ref[:WINDOW, pl.ds(start, quarter)].astype(
            jnp.bfloat16
        )
        out_refs[s][pl.ds(first + WINDOW, TAIL), :] = tail
        state_ref[s, slot] = mixed_ref[WINDOW:, pl.ds(start, quarter)].astype(jnp.bfloat16)


def tail_rows(length, landing, width):
    lane = lax.broadcasted_iota(jnp.int32, (TAIL, width), 1)
    facts = jnp.where(lane == 0, length, jnp.where(lane == 1, landing, 0))
    return facts.astype(jnp.float32).astype(jnp.bfloat16)


def near_shapes(slots, width, heads, quarter):
    return [
        jax.ShapeDtypeStruct((slots * WINDOW, width), jnp.bfloat16),
        jax.ShapeDtypeStruct((slots * WINDOW, width), jnp.bfloat16),
        jax.ShapeDtypeStruct((slots * WINDOW, heads), jnp.float32),
        jax.ShapeDtypeStruct((slots * WINDOW, heads), jnp.bfloat16),
        jax.ShapeDtypeStruct((slots * TAIL, quarter), jnp.bfloat16),
    ]


def run_near_home(mp, table, tokens, shards, slots):
    heads = sum(w.shape[1] for w in shards) // 4
    width = tokens.shape[1]
    top = tokens.shape[0] // BLOCK - 1

    def block_map(b, slot, table_ref):
        return (jnp.minimum(table_ref[slots + slot] + b, top), 0)

    local = pl.BlockSpec(memory_space=pltpu.VMEM)
    outs = pl.pallas_call(
        functools.partial(near_home_kernel, len(shards), slots),
        grid_spec=pltpu.PrefetchScalarGridSpec(
            num_scalar_prefetch=1,
            grid=(slots,),
            in_specs=[
                pl.BlockSpec((BLOCK, width), functools.partial(block_map, b)) for b in range(MAXB)
            ]
            + [local] * len(shards),
            out_specs=[local] * 5,
        ),
        out_shape=near_shapes(slots, width, heads, width // mp),
        compiler_params=LIMIT,
        name="near_home",
    )(table, *([tokens] * MAXB), *shards)
    return [in_vmem(out) for out in outs]


def run_near_owner(mp, arrived, shards, slots):
    heads = sum(w.shape[1] for w in shards) // 4
    width = arrived.shape[1]
    local = pl.BlockSpec(memory_space=pltpu.VMEM)
    outs = pl.pallas_call(
        functools.partial(near_owner_kernel, len(shards)),
        grid=(slots,),
        in_specs=[local] * (1 + len(shards)),
        out_specs=[local] * 5,
        out_shape=near_shapes(slots, width, heads, width // mp),
        compiler_params=LIMIT,
        name="near_owner",
    )(in_vmem(arrived), *shards)
    return [in_vmem(out) for out in outs]


def run_far(mp, shards, near, w_perm, base, groups, whole):
    width = w_perm.shape[1]
    quarter = width // mp
    size = groups * (WINDOW + TAIL)
    local = pl.BlockSpec(memory_space=pltpu.VMEM)
    shapes = (
        [jax.ShapeDtypeStruct((mp, size, quarter), jnp.bfloat16)]
        if whole
        else [jax.ShapeDtypeStruct((size, quarter), jnp.bfloat16)] * mp
    )
    outs = pl.pallas_call(
        functools.partial(far_kernel, mp, len(shards), base, whole),
        grid=(groups,),
        in_specs=[local] * (len(shards) + 6),
        out_specs=[local] * (len(shapes) + 1),
        scratch_shapes=[pltpu.VMEM((WINDOW + TAIL, width), jnp.float32)],
        out_shape=shapes + [jax.ShapeDtypeStruct((mp, groups, TAIL, quarter), jnp.bfloat16)],
        compiler_params=LIMIT,
        name="far_heads",
    )(*shards, *near, w_perm)
    return (outs[0] if whole else outs[:-1]), outs[-1]


def delta(mp, e, m):
    return e * mp + ((m >> 1) ^ ((m & 1) * (mp - 1)))


def plan_kernel(mp, per_pair, slots, ahead, *refs):
    len_ref, owner_ref, land_ref, start_ref, w_ref, wo_ref, tokens_ref = refs[:7]
    home_ref, table_ref, held_ref, wp_ref = refs[7:11]
    me, mine = lax.axis_index("dp"), lax.axis_index("mp")
    owners = home_ref.shape[0]
    users = len_ref.shape[1]
    chunk = -(-users // per_pair)
    top = tokens_ref.shape[0] // BLOCK - 1

    def clear(o, c):
        for i in range(4 * per_pair):
            home_ref[o, i] = 0
        return c

    lax.fori_loop(0, owners, clear, 0)
    for k in range(per_pair):

        def fill(u, c):
            o = owner_ref[0, u]
            home_ref[o, 4 * k] = len_ref[0, u]
            home_ref[o, 4 * k + 1] = start_ref[0, u]
            home_ref[o, 4 * k + 2] = land_ref[0, u]
            home_ref[o, 4 * k + 3] = u
            return c

        lax.fori_loop(k * chunk, min((k + 1) * chunk, users), fill, 0)
    copies = []
    if ahead:
        ahead_ref, sems = refs[11:]
        for i, (e, k) in enumerate(ahead):
            o = me ^ delta(mp, e, mine)
            first = i * (WINDOW + TAIL)
            ahead_ref[first + WINDOW : first + WINDOW + TAIL, :] = tail_rows(
                home_ref[o, 4 * k], home_ref[o, 4 * k + 2], tokens_ref.shape[1]
            )
            for b in range(MAXB):
                block = jnp.minimum(home_ref[o, 4 * k + 1] + b, top)
                copies.append(
                    pltpu.make_async_copy(
                        tokens_ref.at[pl.ds(pl.multiple_of(block * BLOCK, BLOCK), BLOCK), :],
                        ahead_ref.at[pl.ds(first + b * BLOCK, BLOCK), :],
                        sems.at[i * MAXB + b],
                    )
                )
                copies[-1].start()
    for i, (e, k) in enumerate(slots):
        o = me ^ delta(mp, e, mine)
        for j in range(3):
            table_ref[j * len(slots) + i] = home_ref[o, 4 * k + j]
    held_ref[...] = w_ref[...]
    part = wo_ref.shape[0] // mp
    for s in range(mp):
        start = pl.multiple_of((mine ^ s) * part, part)
        wp_ref[s * part : (s + 1) * part, :] = wo_ref[pl.ds(start, part), :]
    for copy in copies:
        copy.wait()


def plan(dp, mp, per_pair, slots, ahead, tables, w_uvqk, w_out, tokens):
    scalar = pl.BlockSpec(memory_space=pltpu.SMEM)
    local = pl.BlockSpec(memory_space=pltpu.VMEM)
    windows = [jax.ShapeDtypeStruct((len(ahead) * (WINDOW + TAIL), tokens.shape[1]), tokens.dtype)]
    windows = windows if ahead else []
    outs = pl.pallas_call(
        functools.partial(plan_kernel, mp, per_pair, slots, ahead),
        in_specs=[scalar] * len(tables) + [local] * 2 + [pl.BlockSpec(memory_space=pl.ANY)],
        out_specs=[scalar] * 2 + [local] * (2 + len(windows)),
        out_shape=[
            jax.ShapeDtypeStruct((dp, 4 * per_pair), jnp.int32),
            jax.ShapeDtypeStruct((3 * len(slots),), jnp.int32),
            jax.ShapeDtypeStruct(w_uvqk.shape, w_uvqk.dtype),
            jax.ShapeDtypeStruct(w_out.shape, w_out.dtype),
        ]
        + windows,
        scratch_shapes=[pltpu.SemaphoreType.DMA((len(ahead) * MAXB,))] * len(windows),
        compiler_params=LIMIT,
        name="plan_users",
    )(*tables, w_uvqk, w_out, tokens)
    return outs[:4], (outs[4] if ahead else None)


def place_kernel(mp, windows, states, count, home_ref, *refs):
    me, mine = lax.axis_index("dp"), lax.axis_index("mp")
    in_refs = refs[:count]
    out_ref, user_ref, users_ref, gather_ref, facts_ref, sem = refs[count:]
    for i, (array, first) in enumerate(windows):
        row = first + WINDOW
        gather_ref[i : i + 1, :] = (
            in_refs[array][row : row + TAIL, :][0:1].astype(jnp.float32).astype(jnp.int32)
        )
    out_ref[...] = jnp.zeros_like(out_ref)
    copy = pltpu.make_async_copy(gather_ref, facts_ref, sem)
    copy.start()
    users_ref[...] = jnp.zeros_like(users_ref)
    for array, first, j, e, k in states:
        o = me ^ delta(mp, e, mine ^ j)

        @pl.when(home_ref[o, 4 * k] > 0)
        def _():
            users_ref[pl.ds(home_ref[o, 4 * k + 3], 1), :] = in_refs[array][
                first : first + TAIL, :
            ].astype(jnp.float32)[0:1]

    user_ref[...] = users_ref[...].astype(user_ref.dtype)
    copy.wait()
    for i, (array, first) in enumerate(windows):
        for b in range(MAXB):

            @pl.when(facts_ref[i, 0] > b * BLOCK)
            def _():
                row = pl.multiple_of((facts_ref[i, 1] + b) * BLOCK, BLOCK)
                out_ref[pl.ds(row, BLOCK), :] = in_refs[array][
                    first + b * BLOCK : first + (b + 1) * BLOCK, :
                ]


def place(mp, windows, states, home, arrays, rows, users):
    quarter = arrays[0].shape[1]
    local = pl.BlockSpec(memory_space=pltpu.VMEM)
    return pl.pallas_call(
        functools.partial(place_kernel, mp, windows, states, len(arrays)),
        in_specs=[pl.BlockSpec(memory_space=pltpu.SMEM)] + [local] * len(arrays),
        out_specs=[local, local],
        out_shape=[
            jax.ShapeDtypeStruct((rows, quarter), jnp.bfloat16),
            jax.ShapeDtypeStruct((users, quarter), jnp.bfloat16),
        ],
        scratch_shapes=[
            pltpu.VMEM((users, quarter), jnp.float32),
            pltpu.VMEM((len(windows), quarter), jnp.int32),
            pltpu.SMEM((len(windows), quarter), jnp.int32),
            pltpu.SemaphoreType.DMA(()),
        ],
        compiler_params=LIMIT,
        name="place_blocks",
    )(home, *[in_vmem(a) for a in arrays])


def per_device(dp, mp, tokens, w_uvqk, w_out, hist_len, owner, recv_offset, block_start):
    users = hist_len.shape[1]
    per_pair = -(-users // dp)
    rounds = dp // mp
    step = WINDOW + TAIL
    upper, lower = range(rounds // 2, rounds), range(rounds // 2)
    ahead = [(e, k) for e in upper for k in range(per_pair - 1)]
    late = [(e, per_pair - 1) for e in upper]
    local = [(e, k) for e in lower for k in range(per_pair)]
    slots = late + local

    def swap(value, j):
        return lax.ppermute(value, "mp", [(i, i ^ j) for i in range(mp)])

    def send(value, e, j):
        pairs = [
            (d * mp + m, (d ^ delta(mp, e, m)) * mp + (m ^ j)) for d in range(dp) for m in range(mp)
        ]
        return lax.ppermute(value, ("dp", "mp"), pairs)

    arrays, windows, states = [], [], []

    def arrive(array, count):
        windows.extend((len(arrays), i * step) for i in range(count))
        arrays.append(array)

    tokens = in_hbm(tokens)
    held = {0: w_uvqk}
    hop = mp // 2
    while hop >= 1:
        held.update({s + hop: swap(value, hop) for s, value in list(held.items())})
        hop //= 2
    (home, table, held[0], w_perm), windows_ahead = plan(
        dp,
        mp,
        per_pair,
        slots,
        ahead,
        [in_hbm(t) for t in (hist_len, owner, recv_offset, block_start)],
        in_hbm(w_uvqk),
        in_hbm(w_out),
        tokens,
    )
    w_perm = in_vmem(w_perm)
    shards = [in_vmem(held[s]) for s in range(mp)]
    half = max(mp // 2, 1)
    sent = []
    turns = per_pair - 1
    for i in range(len(upper) if ahead else 0):
        part = windows_ahead[i * turns * step : (i + 1) * turns * step]
        sent.append(send(part, upper[i], 0))
    near = run_near_home(mp, table, tokens, shards[:half], len(slots))
    out, late_state = run_far(mp, shards[half:], near, w_perm, 0, len(late), True)
    held_late = []
    for i, (e, _) in enumerate(late):
        held_late.append(send(out[:, i * step : (i + 1) * step], e, 0))
    outs, local_state = run_far(mp, shards[half:], near, w_perm, len(late), len(local), False)
    for e in lower:
        for j in range(mp):
            first = e * per_pair * step
            arrive(send(outs[j][first : first + per_pair * step], e, j), per_pair)
    parts = [late_state, local_state]
    order = slots
    for i, e in enumerate(upper if ahead else ()):
        near = run_near_owner(mp, sent[i], shards[:half], turns)
        outs, state = run_far(mp, shards[half:], near, w_perm, 0, turns, False)
        parts.append(send(state, e, 0))
        order = order + [(e, k) for k in range(turns)]
        for j in range(mp):
            arrive(swap(outs[j], j) if j else outs[j], turns)
    for j in range(mp):
        pieces = [value[j] for value in held_late]
        pieces += [part[j].reshape(-1, part.shape[-1]) for part in parts]
        joined = jnp.concatenate(pieces, 0)
        joined = swap(joined, j) if j else joined
        base = len(late) * step
        states += [
            (len(arrays), base + i * TAIL, j, e, k) for i, (e, k) in enumerate(order)
        ]
        arrive(joined, len(late))
    return place(mp, windows, states, home, arrays, tokens.shape[0], users)


def solution(mesh):
    dp, mp = mesh.shape["dp"], mesh.shape["mp"]
    in_specs = (
        P("dp", None),
        P(None, "mp"),
        P(),
        P("dp", None),
        P("dp", None),
        P("dp", None),
        P("dp", None),
    )
    out_specs = (P("dp", "mp"), P("dp", "mp"))
    return jax.shard_map(
        functools.partial(per_device, dp, mp),
        mesh=mesh,
        in_specs=in_specs,
        out_specs=out_specs,
        check_vma=False,
    )
```

```python
import functools

import jax
import jax.numpy as jnp
from jax import lax
from jax.experimental import pallas as pl
from jax.experimental.pallas import tpu as pltpu
from jax.sharding import PartitionSpec as P


BLOCK = 128
MAXB = 2
HEAD = 128
WINDOW = MAXB * BLOCK
TAIL = 8
EPS = 1e-05
LIMIT = pltpu.CompilerParams(vmem_limit_bytes=24 * 1024 * 1024)


def in_vmem(value):
    return pltpu.with_memory_space_constraint(value, pltpu.VMEM)


def in_hbm(value):
    return pltpu.with_memory_space_constraint(value, pltpu.HBM)


def half_silu(half):
    return half + half * jnp.tanh(half)


def norm_scale(total, squares, width):
    average = total * (1.0 / width)
    variance = squares * (1.0 / width) - average * average
    return average, lax.rsqrt(variance + EPS)


def norm_half(widened):
    average, scale = norm_scale(
        jnp.sum(widened, 1, keepdims=True),
        jnp.sum(widened * widened, 1, keepdims=True),
        widened.shape[1],
    )
    return ((widened - average) * (0.5 * scale)).astype(jnp.bfloat16)


def attend_heads(halved, w_refs):
    row = lax.broadcasted_iota(jnp.int32, (BLOCK, BLOCK), 0)
    col = lax.broadcasted_iota(jnp.int32, (BLOCK, BLOCK), 1)
    causal = col <= row
    half_scale = 0.5 * HEAD ** (-0.5)
    heads = [
        w_ref[:, head * 4 * HEAD : (head + 1) * 4 * HEAD]
        for w_ref in w_refs
        for head in range(w_ref.shape[1] // (4 * HEAD))
    ]
    halves = [jnp.dot(halved, w, preferred_element_type=jnp.float32) for w in heads]
    projs = [half_silu(half).astype(jnp.bfloat16) for half in halves]
    split = [[proj[:, i * HEAD : (i + 1) * HEAD] for i in range(4)] for proj in projs]
    raws = [
        lax.dot_general(q, k, (((1,), (1,)), ((), ())), preferred_element_type=jnp.float32)
        for _, _, q, k in split
    ]
    values = []
    for raw, (_, v, _, _) in zip(raws, split):
        weights = []
        for b in range(MAXB):
            rows = slice(b * BLOCK, (b + 1) * BLOCK)
            act = half_silu(raw[rows, : (b + 1) * BLOCK] * half_scale)
            pieces = [act[:, : b * BLOCK]] if b > 0 else []
            pieces.append(jnp.where(causal, act[:, b * BLOCK :], 0.0))
            if b + 1 < MAXB:
                pieces.append(jnp.zeros((BLOCK, WINDOW - (b + 1) * BLOCK), jnp.float32))
            weights.append(jnp.concatenate(pieces, 1).astype(jnp.bfloat16))
        values.append(jnp.dot(jnp.concatenate(weights, 0), v, preferred_element_type=jnp.float32))
    return values, [u for u, _, _, _ in split]


def near_rows(base, widened, w_refs, out_refs):
    rows_ref, half_ref, value_ref, gate_ref = out_refs
    rows = pl.ds(pl.multiple_of(base * WINDOW, WINDOW), WINDOW)
    halved = norm_half(widened)
    rows_ref[rows, :] = widened.astype(rows_ref.dtype)
    half_ref[rows, :] = halved
    values, gates = attend_heads(halved, w_refs)
    value_ref[rows, :] = jnp.concatenate(values, 1)
    gate_ref[rows, :] = jnp.concatenate(gates, 1)


def near_home_kernel(mp, near, base, total_slots, table_ref, *refs):
    block_refs, w_refs = refs[:MAXB], refs[MAXB : MAXB + near]
    near_refs = refs[MAXB + near :]
    slot = pl.program_id(0)
    if base == 0:
        wo_ref, *near_refs, held_ref, wp_ref = near_refs

        @pl.when(slot == 0)
        def _():
            mine = lax.axis_index("mp")
            held_ref[...] = w_refs[0][...]
            part = wo_ref.shape[0] // mp
            for s in range(mp):
                start = pl.multiple_of((mine ^ s) * part, part)
                wp_ref[s * part : (s + 1) * part, :] = wo_ref[pl.ds(start, part), :]

    tail_ref = near_refs[-1]
    tail_ref[pl.ds(pl.multiple_of(slot * TAIL, TAIL), TAIL), :] = tail_rows(
        table_ref[base + slot], table_ref[2 * total_slots + base + slot], tail_ref.shape[1]
    )
    widened = jnp.concatenate([ref[...] for ref in block_refs], 0).astype(jnp.float32)
    near_rows(slot, widened, w_refs, near_refs[:-1])


def near_owner_kernel(near, *refs):
    arrived_ref, w_refs = refs[0], refs[1 : 1 + near]
    tail_ref = refs[-1]
    slot = pl.program_id(0)
    first = pl.multiple_of(slot * (WINDOW + TAIL), TAIL)
    tail_ref[pl.ds(pl.multiple_of(slot * TAIL, TAIL), TAIL), :] = arrived_ref[
        pl.ds(first + WINDOW, TAIL), : tail_ref.shape[1]
    ]
    near_rows(slot, arrived_ref[pl.ds(first, WINDOW), :].astype(jnp.float32), w_refs, refs[1 + near : -1])


def far_kernel(mp, far, base, paired, joined, riders, *refs):
    w_refs = refs[:far]
    rows_ref, half_ref, near_value_ref, near_gate_ref, tail_ref, wp_ref = refs[far : far + 6]
    stated = paired is not False
    earlier = refs[far + 6 : far + 6 + (mp if joined else 0)]
    taken = far + 6 + len(earlier)
    rider_refs = refs[taken : taken + riders]
    out_refs = refs[taken + riders : -2]
    state_ref, mixed_ref = refs[-2:]
    if not stated:
        out_refs, state_ref = refs[taken + riders : -1], None
    if paired:
        out_refs = [out_refs[s // 2].at[s % 2] for s in range(mp)]
    for out_ref, early_ref in zip(out_refs, earlier):
        out_ref[: joined * (WINDOW + TAIL), :] = early_ref[...]
    row = (joined + pl.num_programs(0)) * (WINDOW + TAIL) if riders else 0
    for rider_ref in rider_refs:
        for i in range(rider_ref.shape[1]):
            for s in range(mp):
                out_refs[s][pl.ds(pl.multiple_of(row, TAIL), TAIL), :] = rider_ref[s, i]
            row += TAIL
    slot = pl.program_id(0)
    mine = lax.axis_index("mp")
    width = wp_ref.shape[0]
    rows = pl.ds(pl.multiple_of((base + slot) * WINDOW, WINDOW), WINDOW)
    tail = tail_ref[pl.ds(pl.multiple_of((base + slot) * TAIL, TAIL), TAIL), :]
    length = tail.astype(jnp.float32)[0:1, 0:1]
    values, gates = attend_heads(half_ref[rows, :], w_refs)
    value = jnp.concatenate([near_value_ref[rows, :]] + values, 1)
    gate = jnp.concatenate([near_gate_ref[rows, :]] + gates, 1)
    average, scale = norm_scale(
        jnp.sum(value, 1, keepdims=True) * (1.0 / WINDOW),
        jnp.sum(value * value, 1, keepdims=True) * (1.0 / WINDOW**2),
        width,
    )
    average, scale = average * WINDOW, scale * (1.0 / WINDOW)
    gated = (value - average) * scale * gate.astype(jnp.float32)
    widened = rows_ref[rows, :].astype(jnp.float32)
    live = lax.broadcasted_iota(jnp.int32, (WINDOW, 1), 0).astype(jnp.float32)
    final = live == length - 1.0
    quarter = width // mp
    if paired is None:
        last_gated = jnp.sum(jnp.where(final, gated, 0.0), 0, keepdims=True)
        last_row = jnp.sum(jnp.where(final, widened, 0.0), 0, keepdims=True)
        mixed_ref[WINDOW:, :] = jnp.broadcast_to(last_row, (TAIL, width)) + jnp.dot(
            jnp.broadcast_to(last_gated, (TAIL, width)).astype(jnp.bfloat16),
            wp_ref[...],
            preferred_element_type=jnp.float32,
        )
        for s in range(mp):
            start = pl.multiple_of((mine ^ s) * quarter, quarter)
            state_ref[s, slot] = mixed_ref[WINDOW:, pl.ds(start, quarter)].astype(jnp.bfloat16)
        return
    mixed = widened + jnp.dot(
        gated.astype(jnp.bfloat16), wp_ref[...], preferred_element_type=jnp.float32
    )
    mixed_ref[:WINDOW, :] = jnp.where(live < length, mixed, 0.0)
    last_row = jnp.sum(jnp.where(final, mixed, 0.0), 0, keepdims=True)
    mixed_ref[WINDOW:, :] = jnp.broadcast_to(last_row, (TAIL, width))
    first = pl.multiple_of((joined + slot) * (WINDOW + TAIL), TAIL)
    for s in range(mp):
        start = pl.multiple_of((mine ^ s) * quarter, quarter)
        out_refs[s][pl.ds(first, WINDOW), :] = mixed_ref[:WINDOW, pl.ds(start, quarter)].astype(
            jnp.bfloat16
        )
        out_refs[s][pl.ds(first + WINDOW, TAIL), :] = tail
        if stated:
            state_ref[s, slot] = mixed_ref[WINDOW:, pl.ds(start, quarter)].astype(jnp.bfloat16)


def tail_rows(length, landing, width):
    lane = lax.broadcasted_iota(jnp.int32, (TAIL, width), 1)
    facts = jnp.where(lane == 0, length, jnp.where(lane == 1, landing, 0))
    return facts.astype(jnp.float32).astype(jnp.bfloat16)


def near_shapes(slots, width, heads, quarter):
    return [
        jax.ShapeDtypeStruct((slots * WINDOW, width), jnp.bfloat16),
        jax.ShapeDtypeStruct((slots * WINDOW, width), jnp.bfloat16),
        jax.ShapeDtypeStruct((slots * WINDOW, heads), jnp.float32),
        jax.ShapeDtypeStruct((slots * WINDOW, heads), jnp.bfloat16),
        jax.ShapeDtypeStruct((slots * TAIL, quarter), jnp.bfloat16),
    ]


def run_near_home(mp, table, tokens, shards, base, slots, w_out=None):
    heads = sum(w.shape[1] for w in shards) // 4
    width = tokens.shape[1]
    top = tokens.shape[0] // BLOCK - 1
    total_slots = table.shape[0] // 3
    more = [] if w_out is None else [w_out]
    extra = [] if w_out is None else [shards[0], w_out]

    def block_map(b, slot, table_ref):
        return (jnp.minimum(table_ref[total_slots + base + slot] + b, top), 0)

    local = pl.BlockSpec(memory_space=pltpu.VMEM)
    outs = pl.pallas_call(
        functools.partial(near_home_kernel, mp, len(shards), base, total_slots),
        grid_spec=pltpu.PrefetchScalarGridSpec(
            num_scalar_prefetch=1,
            grid=(slots,),
            in_specs=[
                pl.BlockSpec((BLOCK, width), functools.partial(block_map, b)) for b in range(MAXB)
            ]
            + [local] * (len(shards) + len(more)),
            out_specs=[local] * (5 + len(extra)),
        ),
        out_shape=near_shapes(slots, width, heads, width // mp)
        + [jax.ShapeDtypeStruct(a.shape, a.dtype) for a in extra],
        compiler_params=LIMIT,
        name="near_home",
    )(table, *([tokens] * MAXB), *shards, *more)
    outs = [in_vmem(out) for out in outs]
    return outs[:5], outs[5:]


def run_near_owner(mp, arrived, shards, slots):
    heads = sum(w.shape[1] for w in shards) // 4
    width = arrived.shape[1]
    local = pl.BlockSpec(memory_space=pltpu.VMEM)
    outs = pl.pallas_call(
        functools.partial(near_owner_kernel, len(shards)),
        grid=(slots,),
        in_specs=[local] * (1 + len(shards)),
        out_specs=[local] * 5,
        out_shape=near_shapes(slots, width, heads, width // mp),
        compiler_params=LIMIT,
        name="near_owner",
    )(in_vmem(arrived), *shards)
    return [in_vmem(out) for out in outs]


def run_far(mp, shards, near, w_perm, base, groups, paired, earlier=(), riders=()):
    width = w_perm.shape[1]
    quarter = width // mp
    joined = earlier[0].shape[0] // (WINDOW + TAIL) if earlier else 0
    size = (joined + groups) * (WINDOW + TAIL) + sum(r.shape[1] for r in riders) * TAIL
    local = pl.BlockSpec(memory_space=pltpu.VMEM)
    shapes = (
        [jax.ShapeDtypeStruct((2, size, quarter), jnp.bfloat16)] * (mp // 2)
        if paired
        else [jax.ShapeDtypeStruct((size, quarter), jnp.bfloat16)] * (0 if paired is None else mp)
    )
    states = [jax.ShapeDtypeStruct((mp, groups, TAIL, quarter), jnp.bfloat16)]
    states = [] if paired is False else states
    outs = pl.pallas_call(
        functools.partial(far_kernel, mp, len(shards), base, paired, joined, len(riders)),
        grid=(groups,),
        in_specs=[local] * (len(shards) + 6 + len(earlier) + len(riders)),
        out_specs=[local] * (len(shapes) + len(states)),
        scratch_shapes=[pltpu.VMEM((WINDOW + TAIL, width), jnp.float32)],
        out_shape=shapes + states,
        compiler_params=LIMIT,
        name="far_heads",
    )(*shards, *near, w_perm, *[in_vmem(a) for a in (*earlier, *riders)])
    return outs[: len(shapes)], outs[len(shapes) :]


def delta(mp, e, m):
    return e * mp + ((m >> 1) ^ ((m & 1) * (mp - 1)))


def plan_kernel(mp, per_pair, slots, ahead, *refs):
    len_ref, owner_ref, land_ref, start_ref, tokens_ref = refs[:5]
    home_ref, table_ref = refs[5:7]
    me, mine = lax.axis_index("dp"), lax.axis_index("mp")
    owners = home_ref.shape[0]
    users = len_ref.shape[1]
    chunk = -(-users // per_pair)
    top = tokens_ref.shape[0] // BLOCK - 1

    copies = []
    for i, (e, k) in enumerate(ahead):
        o = me ^ delta(mp, e, mine)
        length = start = landing = jnp.int32(0)
        for u in range(k * chunk, min((k + 1) * chunk, users)):
            hit = owner_ref[0, u] == o
            length = jnp.where(hit, len_ref[0, u], length)
            start = jnp.where(hit, start_ref[0, u], start)
            landing = jnp.where(hit, land_ref[0, u], landing)
        ahead_ref, sems = refs[7 + i], refs[-1]
        for b in range(MAXB):
            block = jnp.minimum(start + b, top)
            copies.append(
                pltpu.make_async_copy(
                    tokens_ref.at[pl.ds(pl.multiple_of(block * BLOCK, BLOCK), BLOCK), :],
                    ahead_ref.at[pl.ds(b * BLOCK, BLOCK), :],
                    sems.at[i * MAXB + b],
                )
            )
            copies[-1].start()
        ahead_ref[WINDOW:, :] = tail_rows(length, landing, tokens_ref.shape[1])

    def clear(o, c):
        for i in range(4 * per_pair):
            home_ref[o, i] = 0
        return c

    lax.fori_loop(0, owners, clear, 0)
    for u in range(users):
        k = u // chunk
        o = owner_ref[0, u]
        home_ref[o, 4 * k] = len_ref[0, u]
        home_ref[o, 4 * k + 1] = start_ref[0, u]
        home_ref[o, 4 * k + 2] = land_ref[0, u]
        home_ref[o, 4 * k + 3] = u
    for i, (e, k) in enumerate(slots):
        o = me ^ delta(mp, e, mine)
        for j in range(3):
            table_ref[j * len(slots) + i] = home_ref[o, 4 * k + j]
    for copy in copies:
        copy.wait()


def plan(dp, mp, per_pair, slots, ahead, tables, tokens):
    scalar = pl.BlockSpec(memory_space=pltpu.SMEM)
    local = pl.BlockSpec(memory_space=pltpu.VMEM)
    windows = [jax.ShapeDtypeStruct((WINDOW + TAIL, tokens.shape[1]), tokens.dtype)] * len(ahead)
    outs = pl.pallas_call(
        functools.partial(plan_kernel, mp, per_pair, slots, ahead),
        in_specs=[scalar] * len(tables) + [pl.BlockSpec(memory_space=pl.ANY)],
        out_specs=[scalar] * 2 + [local] * len(windows),
        out_shape=[
            jax.ShapeDtypeStruct((dp, 4 * per_pair), jnp.int32),
            jax.ShapeDtypeStruct((3 * len(slots),), jnp.int32),
        ]
        + windows,
        scratch_shapes=[pltpu.SemaphoreType.DMA((len(ahead) * MAXB,))] if ahead else [],
        compiler_params=LIMIT,
        name="plan_users",
    )(*tables, tokens)
    return outs[:2], outs[2:]


def place_kernel(mp, windows, states, count, home_ref, *refs):
    me, mine = lax.axis_index("dp"), lax.axis_index("mp")
    in_refs = refs[:count]
    out_ref, user_ref, users_ref, gather_ref, facts_ref, sem = refs[count:]
    windows = [
        (in_refs[array] if lead is None else in_refs[array].at[lead], first)
        for array, lead, first in windows
    ]
    for i, (ref, first) in enumerate(windows):
        row = first + WINDOW
        gather_ref[i : i + 1, :] = (
            ref[row : row + TAIL, :][0:1].astype(jnp.float32).astype(jnp.int32)
        )
    users_ref[...] = jnp.zeros_like(users_ref)
    for array, first, j, e, k in states:
        o = me ^ delta(mp, e, mine ^ j)

        @pl.when(home_ref[o, 4 * k] > 0)
        def _():
            users_ref[pl.ds(home_ref[o, 4 * k + 3], 1), :] = in_refs[array][
                first : first + TAIL, :
            ].astype(jnp.float32)[0:1]

    user_ref[...] = users_ref[...].astype(user_ref.dtype)
    copy = pltpu.make_async_copy(gather_ref, facts_ref, sem)
    copy.start()
    out_ref[...] = jnp.zeros_like(out_ref)
    copy.wait()
    for i, (ref, first) in enumerate(windows):
        for b in range(MAXB):

            @pl.when(facts_ref[i, 0] > b * BLOCK)
            def _():
                row = pl.multiple_of((facts_ref[i, 1] + b) * BLOCK, BLOCK)
                out_ref[pl.ds(row, BLOCK), :] = ref[first + b * BLOCK : first + (b + 1) * BLOCK, :]


def place(mp, windows, states, home, arrays, rows, users):
    quarter = arrays[0].shape[-1]
    local = pl.BlockSpec(memory_space=pltpu.VMEM)
    return pl.pallas_call(
        functools.partial(place_kernel, mp, windows, states, len(arrays)),
        in_specs=[pl.BlockSpec(memory_space=pltpu.SMEM)] + [local] * len(arrays),
        out_specs=[local, local],
        out_shape=[
            jax.ShapeDtypeStruct((rows, quarter), jnp.bfloat16),
            jax.ShapeDtypeStruct((users, quarter), jnp.bfloat16),
        ],
        scratch_shapes=[
            pltpu.VMEM((users, quarter), jnp.float32),
            pltpu.VMEM((len(windows), quarter), jnp.int32),
            pltpu.SMEM((len(windows), quarter), jnp.int32),
            pltpu.SemaphoreType.DMA(()),
        ],
        compiler_params=LIMIT,
        name="place_blocks",
    )(home, *[in_vmem(a) for a in arrays])


def per_device(dp, mp, tokens, w_uvqk, w_out, hist_len, owner, recv_offset, block_start):
    users = hist_len.shape[1]
    per_pair = -(-users // dp)
    rounds = dp // mp
    step = WINDOW + TAIL
    upper, lower = range(rounds // 2, rounds), range(rounds // 2)
    ahead = [(e, k) for e in upper for k in range(per_pair - 1)]
    late = [(e, per_pair - 1) for e in upper]
    local = [(e, k) for e in lower for k in range(per_pair)]
    slots = late + local

    def swap(value, j):
        return lax.ppermute(value, "mp", [(i, i ^ j) for i in range(mp)])

    def send(value, e, j):
        pairs = [
            (d * mp + m, (d ^ delta(mp, e, m)) * mp + (m ^ j)) for d in range(dp) for m in range(mp)
        ]
        return lax.ppermute(value, ("dp", "mp"), pairs)

    arrays, windows, states = [], [], []

    def arrive(array, count, lead=None):
        windows.extend((len(arrays), lead, i * step) for i in range(count))
        arrays.append(array)

    def relay(value, e, j):
        pairs = [
            (d * mp + m, (d ^ delta(mp, e, m ^ j)) * mp + m) for d in range(dp) for m in range(mp)
        ]
        return lax.ppermute(value, ("dp", "mp"), pairs)

    def cross(outs):
        crossed = []
        for p, out in enumerate(outs):
            crossed.append(swap(out, 2 * p) if p else out)
        return crossed

    def send_pairs(outs, jobs, crossed):
        pieces = []
        for e in sorted({e for e, _ in jobs}, reverse=True):
            turns = [i for i, (f, _) in enumerate(jobs) if f == e]
            rows = slice(turns[0] * step, (turns[-1] + 1) * step)
            for p, out in enumerate(outs):
                move = relay if crossed else send
                pieces.append((move(out[:, rows], e, 2 * p), len(turns)))
        return pieces

    def pass_on(pieces):
        for piece, count in pieces:
            arrive(piece, count, 0)
            arrive(swap(piece[1], 1), count)

    tokens = in_hbm(tokens)
    held = {0: w_uvqk}
    hop = mp // 2
    while hop >= 1:
        for shard, value in list(held.items()):
            held[shard + hop] = swap(value, hop)
        hop //= 2
    (home, table), windows_ahead = plan(
        dp,
        mp,
        per_pair,
        slots + ahead,
        ahead,
        [in_hbm(t) for t in (hist_len, owner, recv_offset, block_start)],
        tokens,
    )
    half = max(mp // 2, 1)
    sent = []
    for (e, _), window in zip(ahead, windows_ahead):
        sent.append(send(window, e, 0))
    near, (held[0], w_perm) = run_near_home(
        mp,
        table,
        tokens,
        [in_hbm(w_uvqk)] + [in_vmem(held[s]) for s in range(1, half)],
        0,
        len(slots),
        in_hbm(w_out),
    )
    shards = [in_vmem(held[s]) for s in range(mp)]
    late_outs, (late_state,) = run_far(
        mp, shards[half:], near, w_perm, 0, len(late), True
    )
    late_outs = cross(late_outs)
    outs, (local_state,) = run_far(mp, shards[half:], near, w_perm, len(late), len(local), True)
    local_pieces = send_pairs(outs, local, False)
    late_pieces = send_pairs(late_outs, late, True)
    parts = [late_state, local_state]
    order = slots
    if ahead:
        near = []
        for window in windows_ahead:
            near = run_near_owner(mp, window, shards[:half], 1)
            _, (part,) = run_far(mp, shards[half:], near, w_perm, 0, 1, None)
            parts.append(part)
        order = order + ahead
    earlier = ()
    for i in range(len(ahead)):
        near = run_near_owner(mp, sent[i], shards[:half], 1)
        riders = parts if i + 1 == len(ahead) else ()
        earlier, _ = run_far(mp, shards[half:], near, w_perm, 0, 1, False, earlier, riders)
    base = len(ahead) * step
    for j in range(mp):
        rows = earlier[j] if ahead else jnp.concatenate(
            [part[j].reshape(-1, part.shape[-1]) for part in parts], 0
        )
        states += [(len(arrays), base + i * TAIL, j, e, k) for i, (e, k) in enumerate(order)]
        arrive(swap(rows, j) if j else rows, len(ahead))
    pass_on(local_pieces)
    pass_on(late_pieces)
    return place(mp, windows, states, home, arrays, tokens.shape[0], users)


def solution(mesh):
    dp, mp = mesh.shape["dp"], mesh.shape["mp"]
    in_specs = (
        P("dp", None),
        P(None, "mp"),
        P(),
        P("dp", None),
        P("dp", None),
        P("dp", None),
        P("dp", None),
    )
    out_specs = (P("dp", "mp"), P("dp", "mp"))
    return jax.shard_map(
        functools.partial(per_device, dp, mp),
        mesh=mesh,
        in_specs=in_specs,
        out_specs=out_specs,
        check_vma=False,
    )
```

```python
import functools

import jax
import jax.numpy as jnp
from jax import lax
from jax.experimental import pallas as pl
from jax.experimental.pallas import tpu as pltpu
from jax.sharding import PartitionSpec as P


BLOCK = 128
MAXB = 2
HEAD = 128
WINDOW = MAXB * BLOCK
TAIL = 8
EPS = 1e-05
LIMIT = pltpu.CompilerParams(vmem_limit_bytes=24 * 1024 * 1024)


def in_vmem(value):
    return pltpu.with_memory_space_constraint(value, pltpu.VMEM)


def in_hbm(value):
    return pltpu.with_memory_space_constraint(value, pltpu.HBM)


def half_silu(half):
    return half + half * jnp.tanh(half)


def norm_scale(total, squares, width):
    average = total * (1.0 / width)
    variance = squares * (1.0 / width) - average * average
    return average, lax.rsqrt(variance + EPS)


def norm_half(widened):
    average, scale = norm_scale(
        jnp.sum(widened, 1, keepdims=True),
        jnp.sum(widened * widened, 1, keepdims=True),
        widened.shape[1],
    )
    return ((widened - average) * (0.5 * scale)).astype(jnp.bfloat16)


def attend_heads(halved, w_refs):
    row = lax.broadcasted_iota(jnp.int32, (BLOCK, BLOCK), 0)
    col = lax.broadcasted_iota(jnp.int32, (BLOCK, BLOCK), 1)
    causal = col <= row
    half_scale = 0.5 * HEAD ** (-0.5)
    heads = [
        w_ref[:, head * 4 * HEAD : (head + 1) * 4 * HEAD]
        for w_ref in w_refs
        for head in range(w_ref.shape[1] // (4 * HEAD))
    ]
    halves = [jnp.dot(halved, w, preferred_element_type=jnp.float32) for w in heads]
    projs = [half_silu(half).astype(jnp.bfloat16) for half in halves]
    split = [[proj[:, i * HEAD : (i + 1) * HEAD] for i in range(4)] for proj in projs]
    raws = [
        lax.dot_general(q, k, (((1,), (1,)), ((), ())), preferred_element_type=jnp.float32)
        for _, _, q, k in split
    ]
    values = []
    for raw, (_, v, _, _) in zip(raws, split):
        weights = []
        for b in range(MAXB):
            rows = slice(b * BLOCK, (b + 1) * BLOCK)
            act = half_silu(raw[rows, : (b + 1) * BLOCK] * half_scale)
            pieces = [act[:, : b * BLOCK]] if b > 0 else []
            pieces.append(jnp.where(causal, act[:, b * BLOCK :], 0.0))
            if b + 1 < MAXB:
                pieces.append(jnp.zeros((BLOCK, WINDOW - (b + 1) * BLOCK), jnp.float32))
            weights.append(jnp.concatenate(pieces, 1).astype(jnp.bfloat16))
        values.append(jnp.dot(jnp.concatenate(weights, 0), v, preferred_element_type=jnp.float32))
    return values, [u for u, _, _, _ in split]


def near_rows(base, widened, w_refs, out_refs):
    rows_ref, half_ref, value_ref, gate_ref = out_refs
    rows = pl.ds(pl.multiple_of(base * WINDOW, WINDOW), WINDOW)
    halved = norm_half(widened)
    rows_ref[rows, :] = widened.astype(rows_ref.dtype)
    half_ref[rows, :] = halved
    values, gates = attend_heads(halved, w_refs)
    value_ref[rows, :] = jnp.concatenate(values, 1)
    gate_ref[rows, :] = jnp.concatenate(gates, 1)


def near_home_kernel(mp, near, base, total_slots, table_ref, *refs):
    block_refs, w_refs = refs[:MAXB], refs[MAXB : MAXB + near]
    near_refs = refs[MAXB + near :]
    slot = pl.program_id(0)
    if base == 0:
        wo_ref, *near_refs, held_ref, wp_ref = near_refs

        @pl.when(slot == 0)
        def _():
            mine = lax.axis_index("mp")
            held_ref[...] = w_refs[0][...]
            part = wo_ref.shape[0] // mp
            for s in range(mp):
                start = pl.multiple_of((mine ^ s) * part, part)
                wp_ref[s * part : (s + 1) * part, :] = wo_ref[pl.ds(start, part), :]

    tail_ref = near_refs[-1]
    tail_ref[pl.ds(pl.multiple_of(slot * TAIL, TAIL), TAIL), :] = tail_rows(
        table_ref[base + slot], table_ref[2 * total_slots + base + slot], tail_ref.shape[1]
    )
    widened = jnp.concatenate([ref[...] for ref in block_refs], 0).astype(jnp.float32)
    near_rows(slot, widened, w_refs, near_refs[:-1])


def far_kernel(mp, far, base, fused, paired, joined, riders, *refs):
    w_refs = refs[:far]
    taken = far + (2 if fused else 6)
    near_refs, wp_ref = refs[far : taken - 1], refs[taken - 1]
    stated = paired is not False
    earlier = refs[taken : taken + (mp if joined else 0)]
    taken += len(earlier)
    rider_refs = refs[taken : taken + riders]
    out_refs = refs[taken + riders : -2]
    state_ref, mixed_ref = refs[-2:]
    if not stated:
        out_refs, state_ref = refs[taken + riders : -1], None
    if paired:
        out_refs = [out_refs[s // 2].at[s % 2] for s in range(mp)]
    for out_ref, early_ref in zip(out_refs, earlier):
        out_ref[: joined * (WINDOW + TAIL), :] = early_ref[...]
    row = (joined + pl.num_programs(0)) * (WINDOW + TAIL) if riders else 0
    for rider_ref in rider_refs:
        for i in range(rider_ref.shape[1]):
            for s in range(mp):
                out_refs[s][pl.ds(pl.multiple_of(row, TAIL), TAIL), :] = rider_ref[s, i]
            row += TAIL
    slot = pl.program_id(0)
    mine = lax.axis_index("mp")
    width = wp_ref.shape[0]
    if fused:
        (window_ref,) = near_refs
        tail = window_ref[WINDOW:, : width // mp]
        widened = window_ref[:WINDOW, :].astype(jnp.float32)
        values, gates = attend_heads(norm_half(widened), w_refs)
        value, gate = jnp.concatenate(values, 1), jnp.concatenate(gates, 1)
    else:
        rows_ref, half_ref, near_value_ref, near_gate_ref, tail_ref = near_refs
        rows = pl.ds(pl.multiple_of((base + slot) * WINDOW, WINDOW), WINDOW)
        tail = tail_ref[pl.ds(pl.multiple_of((base + slot) * TAIL, TAIL), TAIL), :]
        widened = rows_ref[rows, :].astype(jnp.float32)
        values, gates = attend_heads(half_ref[rows, :], w_refs)
        value = jnp.concatenate([near_value_ref[rows, :]] + values, 1)
        gate = jnp.concatenate([near_gate_ref[rows, :]] + gates, 1)
    length = tail.astype(jnp.float32)[0:1, 0:1]
    average, scale = norm_scale(
        jnp.sum(value, 1, keepdims=True) * (1.0 / WINDOW),
        jnp.sum(value * value, 1, keepdims=True) * (1.0 / WINDOW**2),
        width,
    )
    average, scale = average * WINDOW, scale * (1.0 / WINDOW)
    gated = (value - average) * scale * gate.astype(jnp.float32)
    live = lax.broadcasted_iota(jnp.int32, (WINDOW, 1), 0).astype(jnp.float32)
    final = live == length - 1.0
    quarter = width // mp
    if paired is None:
        last_gated = jnp.sum(jnp.where(final, gated, 0.0), 0, keepdims=True)
        last_row = jnp.sum(jnp.where(final, widened, 0.0), 0, keepdims=True)
        mixed_ref[WINDOW:, :] = jnp.broadcast_to(last_row, (TAIL, width)) + jnp.dot(
            jnp.broadcast_to(last_gated, (TAIL, width)).astype(jnp.bfloat16),
            wp_ref[...],
            preferred_element_type=jnp.float32,
        )
        for s in range(mp):
            start = pl.multiple_of((mine ^ s) * quarter, quarter)
            state_ref[s, slot] = mixed_ref[WINDOW:, pl.ds(start, quarter)].astype(jnp.bfloat16)
        return
    mixed = widened + jnp.dot(
        gated.astype(jnp.bfloat16), wp_ref[...], preferred_element_type=jnp.float32
    )
    mixed_ref[:WINDOW, :] = jnp.where(live < length, mixed, 0.0)
    last_row = jnp.sum(jnp.where(final, mixed, 0.0), 0, keepdims=True)
    mixed_ref[WINDOW:, :] = jnp.broadcast_to(last_row, (TAIL, width))
    first = pl.multiple_of((joined + slot) * (WINDOW + TAIL), TAIL)
    for s in range(mp):
        start = pl.multiple_of((mine ^ s) * quarter, quarter)
        out_refs[s][pl.ds(first, WINDOW), :] = mixed_ref[:WINDOW, pl.ds(start, quarter)].astype(
            jnp.bfloat16
        )
        out_refs[s][pl.ds(first + WINDOW, TAIL), :] = tail
        if stated:
            state_ref[s, slot] = mixed_ref[WINDOW:, pl.ds(start, quarter)].astype(jnp.bfloat16)


def tail_rows(length, landing, width):
    lane = lax.broadcasted_iota(jnp.int32, (TAIL, width), 1)
    facts = jnp.where(lane == 0, length, jnp.where(lane == 1, landing, 0))
    return facts.astype(jnp.float32).astype(jnp.bfloat16)


def near_shapes(slots, width, heads, quarter):
    return [
        jax.ShapeDtypeStruct((slots * WINDOW, width), jnp.bfloat16),
        jax.ShapeDtypeStruct((slots * WINDOW, width), jnp.bfloat16),
        jax.ShapeDtypeStruct((slots * WINDOW, heads), jnp.float32),
        jax.ShapeDtypeStruct((slots * WINDOW, heads), jnp.bfloat16),
        jax.ShapeDtypeStruct((slots * TAIL, quarter), jnp.bfloat16),
    ]


def run_near_home(mp, table, tokens, shards, base, slots, w_out=None):
    heads = sum(w.shape[1] for w in shards) // 4
    width = tokens.shape[1]
    top = tokens.shape[0] // BLOCK - 1
    total_slots = table.shape[0] // 3
    more = [] if w_out is None else [w_out]
    extra = [] if w_out is None else [shards[0], w_out]

    def block_map(b, slot, table_ref):
        return (jnp.minimum(table_ref[total_slots + base + slot] + b, top), 0)

    local = pl.BlockSpec(memory_space=pltpu.VMEM)
    outs = pl.pallas_call(
        functools.partial(near_home_kernel, mp, len(shards), base, total_slots),
        grid_spec=pltpu.PrefetchScalarGridSpec(
            num_scalar_prefetch=1,
            grid=(slots,),
            in_specs=[
                pl.BlockSpec((BLOCK, width), functools.partial(block_map, b)) for b in range(MAXB)
            ]
            + [local] * (len(shards) + len(more)),
            out_specs=[local] * (5 + len(extra)),
        ),
        out_shape=near_shapes(slots, width, heads, width // mp)
        + [jax.ShapeDtypeStruct(a.shape, a.dtype) for a in extra],
        compiler_params=LIMIT,
        name="near_home",
    )(table, *([tokens] * MAXB), *shards, *more)
    outs = [in_vmem(out) for out in outs]
    return outs[:5], outs[5:]


def run_far(mp, shards, near, w_perm, base, groups, paired, earlier=(), riders=()):
    width = w_perm.shape[1]
    quarter = width // mp
    joined = earlier[0].shape[0] // (WINDOW + TAIL) if earlier else 0
    size = (joined + groups) * (WINDOW + TAIL) + sum(r.shape[1] for r in riders) * TAIL
    local = pl.BlockSpec(memory_space=pltpu.VMEM)
    shapes = (
        [jax.ShapeDtypeStruct((2, size, quarter), jnp.bfloat16)] * (mp // 2)
        if paired
        else [jax.ShapeDtypeStruct((size, quarter), jnp.bfloat16)] * (0 if paired is None else mp)
    )
    states = [jax.ShapeDtypeStruct((mp, groups, TAIL, quarter), jnp.bfloat16)]
    states = [] if paired is False else states
    outs = pl.pallas_call(
        functools.partial(far_kernel, mp, len(shards), base, len(near) == 1, paired, joined, len(riders)),
        grid=(groups,),
        in_specs=[local] * (len(shards) + len(near) + 1 + len(earlier) + len(riders)),
        out_specs=[local] * (len(shapes) + len(states)),
        scratch_shapes=[pltpu.VMEM((WINDOW + TAIL, width), jnp.float32)],
        out_shape=shapes + states,
        compiler_params=LIMIT,
        name="far_heads",
    )(*shards, *near, w_perm, *[in_vmem(a) for a in (*earlier, *riders)])
    return outs[: len(shapes)], outs[len(shapes) :]


def delta(mp, e, m):
    return e * mp + ((m >> 1) ^ ((m & 1) * (mp - 1)))


def plan_kernel(mp, per_pair, slots, ahead, *refs):
    len_ref, owner_ref, land_ref, start_ref, tokens_ref = refs[:5]
    home_ref, table_ref = refs[5:7]
    me, mine = lax.axis_index("dp"), lax.axis_index("mp")
    owners = home_ref.shape[0]
    users = len_ref.shape[1]
    chunk = -(-users // per_pair)
    top = tokens_ref.shape[0] // BLOCK - 1

    copies = []
    for i, (e, k) in enumerate(ahead):
        o = me ^ delta(mp, e, mine)
        length = start = landing = jnp.int32(0)
        for u in range(k * chunk, min((k + 1) * chunk, users)):
            hit = owner_ref[0, u] == o
            length = jnp.where(hit, len_ref[0, u], length)
            start = jnp.where(hit, start_ref[0, u], start)
            landing = jnp.where(hit, land_ref[0, u], landing)
        ahead_ref, sems = refs[7 + i], refs[-1]
        for b in range(MAXB):
            block = jnp.minimum(start + b, top)
            copies.append(
                pltpu.make_async_copy(
                    tokens_ref.at[pl.ds(pl.multiple_of(block * BLOCK, BLOCK), BLOCK), :],
                    ahead_ref.at[pl.ds(b * BLOCK, BLOCK), :],
                    sems.at[i * MAXB + b],
                )
            )
            copies[-1].start()
        ahead_ref[WINDOW:, :] = tail_rows(length, landing, tokens_ref.shape[1])

    def clear(o, c):
        for i in range(4 * per_pair):
            home_ref[o, i] = 0
        return c

    lax.fori_loop(0, owners, clear, 0)
    for u in range(users):
        k = u // chunk
        o = owner_ref[0, u]
        home_ref[o, 4 * k] = len_ref[0, u]
        home_ref[o, 4 * k + 1] = start_ref[0, u]
        home_ref[o, 4 * k + 2] = land_ref[0, u]
        home_ref[o, 4 * k + 3] = u
    for i, (e, k) in enumerate(slots):
        o = me ^ delta(mp, e, mine)
        for j in range(3):
            table_ref[j * len(slots) + i] = home_ref[o, 4 * k + j]
    for copy in copies:
        copy.wait()


def plan(dp, mp, per_pair, slots, ahead, tables, tokens):
    scalar = pl.BlockSpec(memory_space=pltpu.SMEM)
    local = pl.BlockSpec(memory_space=pltpu.VMEM)
    windows = [jax.ShapeDtypeStruct((WINDOW + TAIL, tokens.shape[1]), tokens.dtype)] * len(ahead)
    outs = pl.pallas_call(
        functools.partial(plan_kernel, mp, per_pair, slots, ahead),
        in_specs=[scalar] * len(tables) + [pl.BlockSpec(memory_space=pl.ANY)],
        out_specs=[scalar] * 2 + [local] * len(windows),
        out_shape=[
            jax.ShapeDtypeStruct((dp, 4 * per_pair), jnp.int32),
            jax.ShapeDtypeStruct((3 * len(slots),), jnp.int32),
        ]
        + windows,
        scratch_shapes=[pltpu.SemaphoreType.DMA((len(ahead) * MAXB,))] if ahead else [],
        compiler_params=LIMIT,
        name="plan_users",
    )(*tables, tokens)
    return outs[:2], outs[2:]


def place_kernel(mp, windows, states, count, home_ref, *refs):
    me, mine = lax.axis_index("dp"), lax.axis_index("mp")
    in_refs = refs[:count]
    out_ref, user_ref, users_ref, gather_ref, facts_ref, taken_ref, zero_ref, rounded_ref, sems = refs[count:]
    blocks = out_ref.shape[0] // BLOCK
    windows = [
        (in_refs[array] if lead is None else in_refs[array].at[lead], first)
        for array, lead, first in windows
    ]
    for i, (ref, first) in enumerate(windows):
        row = first + WINDOW
        gather_ref[i : i + 1, :] = (
            ref[row : row + TAIL, :][0:1].astype(jnp.float32).astype(jnp.int32)
        )
    facts = pltpu.make_async_copy(gather_ref, facts_ref, sems.at[0])
    zero_ref[...] = jnp.zeros_like(zero_ref)
    for i in range(blocks):
        taken_ref[i] = 0
    facts.start()
    users_ref[...] = jnp.zeros_like(users_ref)
    for array, first, j, e, k in states:
        o = me ^ delta(mp, e, mine ^ j)

        @pl.when(home_ref[o, 4 * k] > 0)
        def _():
            users_ref[pl.ds(home_ref[o, 4 * k + 3], 1), :] = in_refs[array][
                first : first + TAIL, :
            ].astype(jnp.float32)[0:1]

    rounded_ref[...] = users_ref[...].astype(user_ref.dtype)
    state_copy = pltpu.make_async_copy(rounded_ref, user_ref, sems.at[2])
    state_copy.start()
    facts.wait()
    for i, (ref, first) in enumerate(windows):
        length, block = facts_ref[i, 0], facts_ref[i, 1]
        for b in range(MAXB):

            @pl.when((length > b * BLOCK) & (length <= (b + 1) * BLOCK))
            def _():
                for c in range(b + 1):
                    taken_ref[block + c] = 1
                size = (b + 1) * BLOCK
                pltpu.make_async_copy(
                    ref.at[pl.ds(first, size), :],
                    out_ref.at[pl.ds(pl.multiple_of(block * BLOCK, BLOCK), size), :],
                    sems.at[1],
                ).start()

    def fill(i, c):
        @pl.when(taken_ref[i] == 0)
        def _():
            pltpu.make_async_copy(
                zero_ref,
                out_ref.at[pl.ds(pl.multiple_of(i * BLOCK, BLOCK), BLOCK), :],
                sems.at[1],
            ).start()

        return c

    lax.fori_loop(0, blocks, fill, 0)
    pltpu.make_async_copy(out_ref, out_ref, sems.at[1]).wait()
    state_copy.wait()


def place(mp, windows, states, home, arrays, rows, users):
    quarter = arrays[0].shape[-1]
    local = pl.BlockSpec(memory_space=pltpu.VMEM)
    return pl.pallas_call(
        functools.partial(place_kernel, mp, windows, states, len(arrays)),
        in_specs=[pl.BlockSpec(memory_space=pltpu.SMEM)] + [local] * len(arrays),
        out_specs=[pl.BlockSpec(memory_space=pl.ANY)] * 2,
        out_shape=[
            jax.ShapeDtypeStruct((rows, quarter), jnp.bfloat16),
            jax.ShapeDtypeStruct((users, quarter), jnp.bfloat16),
        ],
        scratch_shapes=[
            pltpu.VMEM((users, quarter), jnp.float32),
            pltpu.VMEM((len(windows), quarter), jnp.int32),
            pltpu.SMEM((len(windows), quarter), jnp.int32),
            pltpu.SMEM((rows // BLOCK,), jnp.int32),
            pltpu.VMEM((BLOCK, quarter), jnp.bfloat16),
            pltpu.VMEM((users, quarter), jnp.bfloat16),
            pltpu.SemaphoreType.DMA((3,)),
        ],
        compiler_params=LIMIT,
        name="place_blocks",
    )(home, *[in_vmem(a) for a in arrays])


def per_device(dp, mp, tokens, w_uvqk, w_out, hist_len, owner, recv_offset, block_start):
    users = hist_len.shape[1]
    per_pair = -(-users // dp)
    rounds = dp // mp
    step = WINDOW + TAIL
    upper, lower = range(rounds // 2, rounds), range(rounds // 2)
    ahead = [(e, k) for e in upper for k in range(per_pair - 1)]
    late = [(e, per_pair - 1) for e in upper]
    local = [(e, k) for e in lower for k in range(per_pair)]
    slots = late + local

    def swap(value, j):
        return lax.ppermute(value, "mp", [(i, i ^ j) for i in range(mp)])

    def send(value, e, j):
        pairs = [
            (d * mp + m, (d ^ delta(mp, e, m)) * mp + (m ^ j)) for d in range(dp) for m in range(mp)
        ]
        return lax.ppermute(value, ("dp", "mp"), pairs)

    arrays, windows, states = [], [], []

    def arrive(array, count, lead=None):
        windows.extend((len(arrays), lead, i * step) for i in range(count))
        arrays.append(array)

    def relay(value, e, j):
        pairs = [
            (d * mp + m, (d ^ delta(mp, e, m ^ j)) * mp + m) for d in range(dp) for m in range(mp)
        ]
        return lax.ppermute(value, ("dp", "mp"), pairs)

    def cross(outs):
        crossed = []
        for p, out in enumerate(outs):
            crossed.append(swap(out, 2 * p) if p else out)
        return crossed

    def send_pairs(outs, jobs, crossed):
        pieces = []
        for e in sorted({e for e, _ in jobs}, reverse=True):
            turns = [i for i, (f, _) in enumerate(jobs) if f == e]
            rows = slice(turns[0] * step, (turns[-1] + 1) * step)
            for p, out in enumerate(outs):
                move = relay if crossed else send
                pieces.append((move(out[:, rows], e, 2 * p), len(turns)))
        return pieces

    def pass_on(pieces):
        for piece, count in pieces:
            arrive(piece, count, 0)
            arrive(swap(piece[1], 1), count)

    tokens = in_hbm(tokens)
    held = {0: w_uvqk}
    hop = mp // 2
    while hop >= 1:
        for shard, value in list(held.items()):
            held[shard + hop] = swap(value, hop)
        hop //= 2
    (home, table), windows_ahead = plan(
        dp,
        mp,
        per_pair,
        slots + ahead,
        ahead,
        [in_hbm(t) for t in (hist_len, owner, recv_offset, block_start)],
        tokens,
    )
    half = max(mp // 2, 1)
    sent = []
    for (e, _), window in zip(ahead, windows_ahead):
        sent.append(send(window, e, 0))
    near, (held[0], w_perm) = run_near_home(
        mp,
        table,
        tokens,
        [in_hbm(w_uvqk)] + [in_vmem(held[s]) for s in range(1, half)],
        0,
        len(slots),
        in_hbm(w_out),
    )
    shards = [in_vmem(held[s]) for s in range(mp)]
    late_outs, (late_state,) = run_far(
        mp, shards[half:], near, w_perm, 0, len(late), True
    )
    late_outs = cross(late_outs)
    outs, (local_state,) = run_far(mp, shards[half:], near, w_perm, len(late), len(local), True)
    local_pieces = send_pairs(outs, local, False)
    late_pieces = send_pairs(late_outs, late, True)
    parts = [late_state, local_state]
    order = slots
    if ahead:
        for window in windows_ahead:
            _, (part,) = run_far(
                mp, shards, [in_vmem(window)], w_perm, 0, 1, None
            )
            parts.append(part)
        order = order + ahead
    earlier = ()
    for i in range(len(ahead)):
        riders = parts if i + 1 == len(ahead) else ()
        earlier, _ = run_far(mp, shards, [in_vmem(sent[i])], w_perm, 0, 1, False, earlier, riders)
    base = len(ahead) * step
    for j in range(mp):
        rows = earlier[j] if ahead else jnp.concatenate(
            [part[j].reshape(-1, part.shape[-1]) for part in parts], 0
        )
        states += [(len(arrays), base + i * TAIL, j, e, k) for i, (e, k) in enumerate(order)]
        arrive(swap(rows, j) if j else rows, len(ahead))
    pass_on(local_pieces)
    pass_on(late_pieces)
    return place(mp, windows, states, home, arrays, tokens.shape[0], users)


def solution(mesh):
    dp, mp = mesh.shape["dp"], mesh.shape["mp"]
    in_specs = (
        P("dp", None),
        P(None, "mp"),
        P(),
        P("dp", None),
        P("dp", None),
        P("dp", None),
        P("dp", None),
    )
    out_specs = (P("dp", "mp"), P("dp", "mp"))
    return jax.shard_map(
        functools.partial(per_device, dp, mp),
        mesh=mesh,
        in_specs=in_specs,
        out_specs=out_specs,
        check_vma=False,
    )
```
